32 devices in a mesh: gx: 8 (over z, x), yz: 4 (over y, core).
Axes of the slice: x: 2, y: 2, z: 4, core: 2. Of those that a mesh axis runs over, the one named last changes fastest.
Arguments:
- state: float32 [4, 256, 192, 256], P(None, 'gx', 'yz'), may hold values from -6 to 6
- mean_flow: float32 [256, 192, 256], P('gx', 'yz'), may hold values from 0.2 to 1.2
- face_cell: int32 [6144], P(('gx', 'yz')), may hold values from 0 to 12582911, as said below
- face_normal: float32 [3, 6144], P(None, ('gx', 'yz')), may hold values from -3 to 3
- face_pos: float32 [3, 6144], P(None, ('gx', 'yz')), may hold values from -2 to 2
- observer_pos: float32 [3, 512], replicated, may hold values from 4 to 12
- time_bin: int32 [6144, 512], P(('gx', 'yz')), may hold values from 0 to 63
Outputs:
- state_next: float32 [4, 256, 192, 256], P(None, 'gx', 'yz')
- signal: float32 [512, 64], P(('gx', 'yz'))
The draws below stay inside these ranges and needn't reach their ends.
Inputs may be any that keep to these rules, and one draw needn't show every extreme that they name: `face_cell`: face j is held by device j // 192 of gx+yz, and its cell, numbered (x 192 + y) * 256 + z, lies in that device's block of grid cells.
All inputs are finite; a program needn't handle non-finite values.
Results may differ from the reference program's by a relative error of at most 0.000084.
Values sent between devices are 32-bit elements; how exact they have to be, the bound alone decides.
A program may use at most 192 MiB of HBM per device.

```python
import jax
import jax.numpy as jnp
from jax import lax

CX = 32
CY = 48
NZ = 256
FACES_DEV = 192
OBS = 512
BINS = 64
NX = 256
NY = 192
FACES = 6144
N_YZ = 4


def draw_face_cell(key, part):
    faces = jnp.arange(FACES, dtype=jnp.int32)
    device = faces // FACES_DEV
    column = device // N_YZ
    group = device % N_YZ
    key_x, key_y, key_z = jax.random.split(key, 3)
    along_x = jax.random.randint(key_x, (FACES,), 0, CX, dtype=jnp.int32)
    along_y = jax.random.randint(key_y, (FACES,), 0, CY, dtype=jnp.int32)
    along_z = jax.random.randint(key_z, (FACES,), 0, NZ, dtype=jnp.int32)
    cell = ((column * CX + along_x) * (CY * N_YZ) + group * CY + along_y) * NZ + along_z
    return cell.astype(jnp.int32)


def with_ends(entries, own_key, least, top_value):
    spot = [jax.random.randint(jax.random.fold_in(own_key, axis), (), 0, length) for axis, length in enumerate(entries.shape)]
    main_axis = entries.shape.index(max(entries.shape))
    beside = spot[:main_axis] + [(spot[main_axis] + 1) % entries.shape[main_axis]] + spot[main_axis + 1:]
    return entries.at[tuple(spot)].set(least).at[tuple(beside)].set(top_value)


def block_scale(stream_key, shape, pieces, least, high):
    loudness = 1.0
    for dim, shards_of in pieces:
        heights = jax.random.uniform(jax.random.fold_in(jax.random.fold_in(stream_key, 6), dim), (shards_of,), jnp.float32, least / len(pieces), high / len(pieces))
        loudness = loudness * jnp.repeat(jnp.exp(heights), shape[dim] // shards_of).reshape((-1,) + (1,) * (len(shape) - 1 - dim))
    return loudness


def bell_draw(own_key, extent, width, limit, shards=(), kind=jnp.bfloat16):
    factor_of = block_scale(own_key, extent, shards, -0.22, 0.18) if shards else 1.0
    array = jax.random.normal(own_key, extent, jnp.float32) * width * factor_of
    return jnp.minimum(jnp.maximum(array, -limit), limit).astype(kind)


def setup_inputs(seed: int = 0) -> dict:
    key_list = jax.random.split(jax.random.key(seed), 8)
    state = bell_draw(key_list[0], (4, NX, NY, NZ), 1.0, 6.0, ((1, 8), (2, 4)), jnp.float32)
    mean_flow = jnp.clip(0.2 + 1 * jax.random.uniform(key_list[1], (NX, NY, NZ), jnp.float32) ** block_scale(key_list[1], (NX, NY, NZ), ((0, 8), (1, 4)), -0.2, 0.2), 0.2, 1.2)
    face_cell = draw_face_cell(jax.random.fold_in(key_list[7], 71), 0)
    face_normal = jnp.clip(jax.random.uniform(key_list[3], (3, FACES), jnp.float32, -3.0, 3.0) * block_scale(key_list[3], (3, FACES), ((1, 32),), -0.4, 0.0), -3.0, 3.0)
    face_pos = jnp.clip(jax.random.uniform(key_list[4], (3, FACES), jnp.float32, -2.0, 2.0) * block_scale(key_list[4], (3, FACES), ((1, 32),), -0.4, 0.0), -2.0, 2.0)
    observer_pos = jnp.clip(jax.random.uniform(key_list[5], (3, OBS), jnp.float32, 4.0, 12.0), 4.0, 12.0)
    time_bin = with_ends(jax.random.randint(key_list[6], (FACES, OBS), 0, BINS), jax.random.fold_in(key_list[6], 1), 0, BINS - 1).astype(jnp.int32)
    return dict(state=state, mean_flow=mean_flow, face_cell=face_cell, face_normal=face_normal, face_pos=face_pos, observer_pos=observer_pos, time_bin=time_bin)


time_step = 0.25
four_pi = 4.0 * 3.141592653589793

def diagonals(count, dtype):
    index = jnp.arange(count)
    third = jnp.full((count,), 1.0 / 3.0, dtype)
    quarter = jnp.asarray(0.25, dtype)
    lower = jnp.where(index == 1, quarter, third)
    lower = jnp.where(index == count - 2, quarter, lower)
    lower = jnp.where(index == count - 1, jnp.asarray(2.0, dtype), lower)
    lower = jnp.where(index == 0, jnp.asarray(0.0, dtype), lower)
    upper = jnp.where(index == 1, quarter, third)
    upper = jnp.where(index == count - 2, quarter, upper)
    upper = jnp.where(index == 0, jnp.asarray(2.0, dtype), upper)
    upper = jnp.where(index == count - 1, jnp.asarray(0.0, dtype), upper)
    return (lower, jnp.ones((count,), dtype), upper)

def compact_rhs(field, axis):
    count = field.shape[axis]
    widths = [(2, 2) if dimension == axis else (0, 0) for dimension in range(field.ndim)]
    padded = jnp.pad(field, widths)

    def take(first, last):
        return lax.slice_in_dim(padded, first, last, axis=axis)

    def plane(index):
        return lax.slice_in_dim(field, index, index + 1, axis=axis)
    inner = 7.0 / 9.0 * (take(3, count + 3) - take(1, count + 1)) + 1.0 / 36.0 * (take(4, count + 4) - take(0, count))
    first_row = 0.5 * (4.0 * plane(1) + plane(2) - 5.0 * plane(0))
    second_row = 0.75 * (plane(2) - plane(0))
    before_last = 0.75 * (plane(count - 1) - plane(count - 3))
    last_row = 0.5 * (5.0 * plane(count - 1) - 4.0 * plane(count - 2) - plane(count - 3))
    middle_rows = lax.slice_in_dim(inner, 2, count - 2, axis=axis)
    return jnp.concatenate([first_row, second_row, middle_rows, before_last, last_row], axis)

def compact_derivative(field, axis):
    moved = jnp.moveaxis(compact_rhs(field, axis), axis, 0)
    count = moved.shape[0]
    lower, middle, upper = diagonals(count, field.dtype)
    solved = lax.linalg.tridiagonal_solve(lower, middle, upper, moved.reshape(count, -1))
    return jnp.moveaxis(solved.reshape(moved.shape), 0, axis)

def explicit_y(field):
    count = field.shape[1]
    padded = jnp.pad(field, ((0, 0), (3, 3), (0, 0)))

    def take(shift):
        return padded[:, 3 + shift:3 + shift + count]
    return 0.75 * (take(1) - take(-1)) - 0.15 * (take(2) - take(-2)) + 1.0 / 60.0 * (take(3) - take(-3))

def reference(state, mean_flow, face_cell, face_normal, face_pos, observer_pos, time_bin):
    pressure, stream, lateral, vertical = (state[0], state[1], state[2], state[3])
    pressure_x = compact_derivative(pressure, 0)
    stream_x = compact_derivative(stream, 0)
    lateral_x = compact_derivative(lateral, 0)
    vertical_x = compact_derivative(vertical, 0)
    mean_x = compact_derivative(mean_flow, 0)
    pressure_y = explicit_y(pressure)
    lateral_y = explicit_y(lateral)
    mean_y = explicit_y(mean_flow)
    pressure_z = compact_derivative(pressure, 2)
    vertical_z = compact_derivative(vertical, 2)
    mean_z = compact_derivative(mean_flow, 2)
    pressure_rate = -(mean_flow * pressure_x + stream_x + lateral_y + vertical_z)
    stream_rate = -(mean_flow * stream_x + stream * mean_x + lateral * mean_y + vertical * mean_z + pressure_x)
    lateral_rate = -(mean_flow * lateral_x + pressure_y)
    vertical_rate = -(mean_flow * vertical_x + pressure_z)
    rates = jnp.stack([pressure_rate, stream_rate, lateral_rate, vertical_rate])
    state_next = state + time_step * rates
    face_rates = rates.reshape(4, -1)[:, face_cell]
    face_pressure = state_next[0].reshape(-1)[face_cell]
    normal_rate = face_normal[0] * face_rates[1] + face_normal[1] * face_rates[2] + face_normal[2] * face_rates[3]
    offset_x = observer_pos[0][None, :] - face_pos[0][:, None]
    offset_y = observer_pos[1][None, :] - face_pos[1][:, None]
    offset_z = observer_pos[2][None, :] - face_pos[2][:, None]
    distance = jnp.sqrt(offset_x * offset_x + offset_y * offset_y + offset_z * offset_z)
    normal_r = (face_normal[0][:, None] * offset_x + face_normal[1][:, None] * offset_y + face_normal[2][:, None] * offset_z) / distance
    contribution = (normal_rate[:, None] + (face_rates[0][:, None] + face_pressure[:, None] / distance) * normal_r) / (four_pi * distance)
    slots = jnp.arange(OBS, dtype=jnp.int32)[None, :] * BINS + time_bin
    signal = jnp.zeros((OBS * BINS,), contribution.dtype).at[slots.reshape(-1)].add(contribution.reshape(-1))
    return (state_next, signal.reshape(OBS, BINS))
```

```python
import functools

import numpy as np
import jax
import jax.numpy as jnp
from jax import lax
from jax.experimental import pallas as pl
from jax.experimental.pallas import tpu as pltpu
from jax.sharding import PartitionSpec as P

BINS = 64
TILE = 8
TAPS = 5

time_step = 0.25
four_pi = 4.0 * 3.141592653589793
VMEM = pltpu.VMEM
SMEM = pltpu.SMEM


def diagonals(count):
    lower = np.full(count, 1.0 / 3.0)
    upper = np.full(count, 1.0 / 3.0)
    lower[1] = lower[count - 2] = upper[1] = upper[count - 2] = 0.25
    lower[0] = upper[count - 1] = 0.0
    lower[count - 1] = upper[0] = 2.0
    return lower, upper


def stencil(count):
    rows = np.zeros((count, count))
    for i in range(2, count - 2):
        rows[i, i + 1], rows[i, i - 1] = 7.0 / 9.0, -7.0 / 9.0
        rows[i, i + 2], rows[i, i - 2] = 1.0 / 36.0, -1.0 / 36.0
    rows[0, :3] = (-2.5, 2.0, 0.5)
    rows[1, 0], rows[1, 2] = -0.75, 0.75
    rows[count - 2, count - 3], rows[count - 2, count - 1] = -0.75, 0.75
    rows[count - 1, count - 3:] = (-0.5, -2.0, 2.5)
    return rows


def dense_derivative(count):
    lower, upper = diagonals(count)
    matrix = np.eye(count) + np.diag(lower[1:], -1) + np.diag(upper[:-1], 1)
    return np.linalg.solve(matrix, stencil(count))


def x_tables(blocks, cells):
    count = blocks * cells
    lower, upper = diagonals(count)
    rows = stencil(count)
    down, pivot = np.zeros(count), np.ones(count)
    for i in range(1, count):
        down[i] = lower[i] / pivot[i - 1]
        pivot[i] = 1.0 - down[i] * upper[i - 1]
    up, pivot_up = np.zeros(count), np.ones(count)
    for i in range(count - 2, -1, -1):
        up[i] = upper[i] / pivot_up[i + 1]
        pivot_up[i] = 1.0 - up[i] * lower[i + 1]
    from_left = rows.copy()
    for i in range(1, count):
        from_left[i] -= down[i] * from_left[i - 1]
    from_right = rows.copy()
    for i in range(count - 2, -1, -1):
        from_right[i] -= up[i] * from_right[i + 1]
    weights = np.zeros((blocks, 2, cells))
    chain = np.zeros((blocks, 2))
    sweep = np.zeros((blocks, 3, cells))
    taps = np.zeros((blocks, 4, TAPS))
    ends = np.zeros((blocks, 4))
    for d in range(blocks):
        s, e = d * cells, (d + 1) * cells
        if d < blocks - 1:
            weights[d, 0] = from_left[e + 1, s:e]
            chain[d, 0] = np.prod(-down[s + 2:e + 2])
        if d > 0:
            weights[d, 1] = from_right[s - 2, s:e]
            chain[d, 1] = np.prod(-up[s - 2:e - 2])
        sweep[d, 0] = down[s:e]
        sweep[d, 1] = 1.0 / pivot[s:e]
        sweep[d, 2] = upper[s:e] / pivot[s:e]
        sweep[d, 1, -1] = 1.0 / (pivot[e - 1] + pivot_up[e - 1] - 1.0)
        taps[d, 0, 2:] = from_left[s, s:s + 3]
        taps[d, 3, :3] = from_right[e - 1, e - 3:e]
        for k in range(-2, 3):
            if 0 <= s + 1 + k:
                taps[d, 1, k + 2] = rows[s + 1, s + 1 + k]
            if e - 2 + k < count:
                taps[d, 2, k + 2] = rows[e - 2, e - 2 + k]
        ends[d, 0] = -1.0 / down[s + 1]
        ends[d, 1] = taps[d, 1, 1] / down[s + 1] if d > 0 else 0.0
        ends[d, 2] = -1.0 / up[e - 2]
        ends[d, 3] = taps[d, 2, 3] / up[e - 2] if d < blocks - 1 else 0.0
        if d > 0:
            ends[d, 1] = rows[s + 1, s - 1] / down[s + 1]
        if d < blocks - 1:
            ends[d, 3] = rows[e - 2, e] / up[e - 2]
    largest, hops, reach = np.abs(chain).max(), 1, np.abs(chain).max()
    while hops < blocks - 1 and reach >= np.finfo(np.float32).tiny:
        hops, reach = hops + 1, reach * largest
    edges = np.concatenate([taps.reshape(blocks, -1), ends], 1)
    return (
        weights.astype(np.float32),
        chain.astype(np.float32),
        sweep.astype(np.float32),
        edges.astype(np.float32),
        hops,
    )


def sums_kernel(cells, weights_ref, state_ref, flow_ref, right_ref, left_ref):
    def load(f, i):
        return flow_ref[i] if f == 4 else state_ref[f, i]

    for f in range(5):
        total_right = weights_ref[0, 0] * load(f, 0)
        total_left = weights_ref[1, 0] * load(f, 0)
        for i in range(1, cells):
            value = load(f, i)
            total_right += weights_ref[0, i] * value
            total_left += weights_ref[1, i] * value
        right_ref[0, f] = total_right
        left_ref[0, f] = total_left
        right_ref[1, f] = load(f, cells - 1)
        left_ref[1, f] = load(f, 0)


def main_kernel(
    cells, width, depth,
    row_ref, sweep_ref, edges_ref,
    state_ref, flow_ref, right_ref, left_ref, low_ref, high_ref,
    zhi_ref, zlo_ref, along_z_ref, normal_ref, pos_ref, observer_ref, bin_ref,
    next_ref, signal_ref,
    wide, swept, zrate, rate, picked,
):
    step = pl.program_id(0)
    rows = pl.ds(pl.multiple_of(step * TILE, TILE), TILE)
    window = pl.ds(pl.multiple_of(step * TILE, TILE), 3 * TILE)

    def load(f, i):
        return flow_ref[i, rows, :] if f == 4 else state_ref[f, i, rows, :]

    @pl.when(step == 0)
    def _():
        def widen(i, carry):
            for slot, f in enumerate((0, 2, 4)):
                body = flow_ref[i] if f == 4 else state_ref[f, i]
                wide[slot, i, TILE:TILE + width, :] = body
                wide[slot, i, TILE - 3:TILE, :] = low_ref[slot, i]
                wide[slot, i, TILE + width:TILE + width + 3, :] = high_ref[slot, i]
            return carry
        lax.fori_loop(0, cells, widen, 0)

    for slot, f in enumerate((0, 3, 4)):
        block = flow_ref[:, rows, :] if f == 4 else state_ref[f, :, rows, :]
        block = block.reshape(cells * TILE, depth)
        high = block.astype(jnp.bfloat16)
        rest = (block - high.astype(jnp.float32)).astype(jnp.bfloat16)
        out = jnp.dot(rest, zhi_ref[...], preferred_element_type=jnp.float32)
        out += jnp.dot(high, zlo_ref[...], preferred_element_type=jnp.float32)
        out += jnp.dot(high, zhi_ref[...], preferred_element_type=jnp.float32)
        zrate[slot] = out.reshape(cells, TILE, depth)

    fields = range(5)

    def tap(k, position):
        return edges_ref[0, k * TAPS + position + 2]

    def end(k):
        return edges_ref[0, 4 * TAPS + k]

    carry = []
    for f in fields:
        first = tap(0, 0) * load(f, 0) + tap(0, 1) * load(f, 1) + tap(0, 2) * load(f, 2)
        value = first + end(0) * right_ref[0, f] + end(1) * right_ref[1, f]
        swept[f, 0] = value
        second = (
            tap(1, -1) * load(f, 0) + tap(1, 0) * load(f, 1)
            + tap(1, 1) * load(f, 2) + tap(1, 2) * load(f, 3) + tap(1, -2) * right_ref[1, f]
        )
        value = second - sweep_ref[0, 1] * value
        swept[f, 1] = value
        carry.append(value)

    def forward(i, carry):
        new = []
        factor = sweep_ref[0, i]
        for f in fields:
            rhs = 7.0 / 9.0 * (load(f, i + 1) - load(f, i - 1)) + 1.0 / 36.0 * (
                load(f, i + 2) - load(f, i - 2)
            )
            value = rhs - factor * carry[f]
            swept[f, i] = value
            new.append(value)
        return tuple(new)

    carry = lax.fori_loop(2, cells - 2, forward, tuple(carry), unroll=2)
    solved = []
    n = cells
    for f in fields:
        before = (
            tap(2, -2) * load(f, n - 4) + tap(2, -1) * load(f, n - 3) + tap(2, 0) * load(f, n - 2)
            + tap(2, 1) * load(f, n - 1) + tap(2, 2) * left_ref[1, f]
        )
        value = before - sweep_ref[0, n - 2] * carry[f]
        swept[f, n - 2] = value
        last = (
            tap(3, -2) * load(f, n - 3) + tap(3, -1) * load(f, n - 2) + tap(3, 0) * load(f, n - 1)
            + end(2) * left_ref[0, f] + end(3) * left_ref[1, f]
        )
        solved.append((last - sweep_ref[0, n - 1] * value) * sweep_ref[1, n - 1])

    def y_rate(slot, i):
        whole = wide[slot, i, window, :]

        def take(shift):
            return whole[TILE + shift:2 * TILE + shift]

        return (
            0.75 * (take(1) - take(-1))
            - 0.15 * (take(2) - take(-2))
            + 1.0 / 60.0 * (take(3) - take(-3))
        )

    def finish(i, x):
        p, u, v, w, flow = (load(f, i) for f in fields)
        rates = (
            -(flow * x[0] + x[1] + y_rate(1, i) + zrate[1, i]),
            -(flow * x[1] + u * x[4] + v * y_rate(2, i) + w * zrate[2, i] + x[0]),
            -(flow * x[2] + y_rate(0, i)),
            -(flow * x[3] + zrate[0, i]),
        )
        place = pl.ds(pl.multiple_of(i * width + step * TILE, TILE), TILE)
        for c, old in enumerate((p, u, v, w)):
            rate[c, place, :] = rates[c]
            new = old + time_step * rates[c]
            next_ref[c, i] = new
            if c == 0:
                rate[4, place, :] = new

    finish(n - 1, solved)

    def backward(k, carry):
        i = n - 2 - k
        x = tuple(
            swept[f, i] * sweep_ref[1, i] - sweep_ref[2, i] * carry[f] for f in fields
        )
        finish(i, x)
        return x

    lax.fori_loop(0, n - 1, backward, tuple(solved))

    @pl.when(step == pl.num_programs(0) - 1)
    def _():
        faces = picked.shape[1]

        def pick(k, carry):
            row = row_ref[0, k]
            for c in range(5):
                picked[c, pl.ds(k, 1), :] = rate[c, pl.ds(row, 1), :]
            return carry

        lax.fori_loop(0, faces, pick, 0, unroll=4)
        mask = lax.broadcasted_iota(jnp.int32, (faces, depth), 1) == along_z_ref[...]
        at = [
            jnp.sum(jnp.where(mask, picked[c], 0.0), axis=1, keepdims=True) for c in range(5)
        ]
        normal = [normal_ref[:, c:c + 1] for c in range(3)]
        normal_rate = normal[0] * at[1] + normal[1] * at[2] + normal[2] * at[3]
        offset = [observer_ref[c:c + 1, :] - pos_ref[:, c:c + 1] for c in range(3)]
        distance = jnp.sqrt(
            offset[0] * offset[0] + offset[1] * offset[1] + offset[2] * offset[2]
        )
        normal_r = (
            normal[0] * offset[0] + normal[1] * offset[1] + normal[2] * offset[2]
        ) / distance
        contribution = (normal_rate + (at[0] + at[4] / distance) * normal_r) / (
            four_pi * distance
        )
        bins = bin_ref[...]

        def gather(b, carry):
            signal_ref[pl.ds(b, 1), :] = jnp.sum(
                jnp.where(bins == b, contribution, 0.0), axis=0, keepdims=True
            )
            return carry

        lax.fori_loop(0, BINS, gather, 0, unroll=2)


def per_device(sizes, state, mean_flow, face_cell, face_normal, face_pos, observer_pos, time_bin):
    blocks, groups = sizes
    _, cells, width, depth = state.shape
    faces, observers = time_bin.shape
    tiles = width // TILE
    block, group = lax.axis_index("gx"), lax.axis_index("yz")
    weights, chain, sweep, edges, hops = x_tables(blocks, cells)

    def mine(table):
        return lax.dynamic_index_in_dim(jnp.asarray(table), block, 0, keepdims=False)

    params = dict(vmem_limit_bytes=60 * 1024 * 1024)
    plane = jax.ShapeDtypeStruct((2, 5, width, depth), jnp.float32)
    plane_spec = pl.BlockSpec((2, 5, TILE, depth), lambda j: (0, 0, j, 0))
    to_right, to_left = pl.pallas_call(
        functools.partial(sums_kernel, cells),
        grid=(tiles,),
        out_shape=(plane, plane),
        in_specs=[
            pl.BlockSpec(memory_space=SMEM),
            pl.BlockSpec((4, cells, TILE, depth), lambda j: (0, 0, j, 0)),
            pl.BlockSpec((cells, TILE, depth), lambda j: (0, j, 0)),
        ],
        out_specs=(plane_spec, plane_spec),
        compiler_params=pltpu.CompilerParams(**params),
    )(mine(weights), state, mean_flow)

    def neighbours(count):
        up = [(i, i + 1) for i in range(count - 1)]
        return up, [(b, a) for a, b in up]

    up, down = neighbours(groups)
    crossing = lambda a, b: jnp.stack(
        [state[0, :, a:b], state[2, :, a:b], mean_flow[:, a:b]]
    )
    low = lax.ppermute(crossing(width - 3, width), "yz", up)
    high = lax.ppermute(crossing(0, 3), "yz", down)
    up, down = neighbours(blocks)
    from_left = lax.ppermute(to_right, "gx", up)
    from_right = lax.ppermute(to_left, "gx", down)
    own = mine(chain)
    sum_left, sum_right = from_left[0], from_right[0]
    for _ in range(hops - 1):
        sum_left = lax.ppermute(to_right[0] + own[0] * sum_left, "gx", up)
        sum_right = lax.ppermute(to_left[0] + own[1] * sum_right, "gx", down)
    from_left = jnp.stack([sum_left, from_left[1]])
    from_right = jnp.stack([sum_right, from_right[1]])

    operator = dense_derivative(depth).T.astype(np.float32)
    z_high = jnp.asarray(operator).astype(jnp.bfloat16)
    z_low = (jnp.asarray(operator) - z_high.astype(jnp.float32)).astype(jnp.bfloat16)

    planes = width * groups
    along_x = face_cell // (planes * depth) - block * cells
    along_y = face_cell // depth % planes - group * width
    along_z = face_cell % depth
    row = (along_x * width + along_y).reshape(1, faces)

    def whole(*shape):
        return pl.BlockSpec(shape, lambda j: (0,) * len(shape))

    smem = pl.BlockSpec(memory_space=SMEM)
    state_next, signal = pl.pallas_call(
        functools.partial(main_kernel, cells, width, depth),
        grid=(tiles,),
        out_shape=(
            jax.ShapeDtypeStruct(state.shape, jnp.float32),
            jax.ShapeDtypeStruct((BINS, observers), jnp.float32),
        ),
        in_specs=[
            smem, smem, smem,
            whole(4, cells, width, depth), whole(cells, width, depth),
            plane_spec, plane_spec,
            whole(3, cells, 3, depth), whole(3, cells, 3, depth),
            whole(depth, depth), whole(depth, depth),
            whole(faces, 1), whole(faces, 3), whole(faces, 3),
            whole(3, observers), whole(faces, observers),
        ],
        out_specs=(
            pl.BlockSpec((4, cells, TILE, depth), lambda j: (0, 0, j, 0)),
            whole(BINS, observers),
        ),
        scratch_shapes=[
            VMEM((3, cells, width + 2 * TILE, depth), jnp.float32),
            VMEM((5, cells, TILE, depth), jnp.float32),
            VMEM((3, cells, TILE, depth), jnp.float32),
            VMEM((5, cells * width, depth), jnp.float32),
            VMEM((5, faces, depth), jnp.float32),
        ],
        compiler_params=pltpu.CompilerParams(**params),
    )(
        row, mine(sweep), mine(edges.reshape(blocks, 1, -1)),
        state, mean_flow, from_left, from_right, low, high,
        z_high, z_low, along_z.reshape(faces, 1), face_normal.T, face_pos.T,
        observer_pos, time_bin,
    )
    devices = blocks * groups
    pieces = signal.T.reshape(devices, -1)
    pieces = lax.all_to_all(pieces, ("gx", "yz"), split_axis=0, concat_axis=0, tiled=True)
    signal = jnp.sum(pieces.reshape(devices, -1), axis=0).reshape(observers // devices, BINS)
    return state_next, signal


def solution(mesh):
    in_specs = (
        P(None, "gx", "yz", None),
        P("gx", "yz", None),
        P(("gx", "yz")),
        P(None, ("gx", "yz")),
        P(None, ("gx", "yz")),
        P(),
        P(("gx", "yz"), None),
    )
    out_specs = (P(None, "gx", "yz", None), P(("gx", "yz"), None))
    sizes = (mesh.shape["gx"], mesh.shape["yz"])
    return jax.shard_map(
        functools.partial(per_device, sizes),
        mesh=mesh, in_specs=in_specs, out_specs=out_specs, check_vma=False,
    )
```

```python
import functools

import numpy as np
import jax
import jax.numpy as jnp
from jax import lax
from jax.experimental import pallas as pl
from jax.experimental.pallas import tpu as pltpu
from jax.sharding import PartitionSpec as P

BINS = 64
TILE = 8
TAPS = 5

time_step = 0.25
four_pi = 4.0 * 3.141592653589793
VMEM = pltpu.VMEM
SMEM = pltpu.SMEM


def diagonals(count):
    lower = np.full(count, 1.0 / 3.0)
    upper = np.full(count, 1.0 / 3.0)
    lower[1] = lower[count - 2] = upper[1] = upper[count - 2] = 0.25
    lower[0] = upper[count - 1] = 0.0
    lower[count - 1] = upper[0] = 2.0
    return lower, upper


def stencil(count):
    rows = np.zeros((count, count))
    for i in range(2, count - 2):
        rows[i, i + 1], rows[i, i - 1] = 7.0 / 9.0, -7.0 / 9.0
        rows[i, i + 2], rows[i, i - 2] = 1.0 / 36.0, -1.0 / 36.0
    rows[0, :3] = (-2.5, 2.0, 0.5)
    rows[1, 0], rows[1, 2] = -0.75, 0.75
    rows[count - 2, count - 3], rows[count - 2, count - 1] = -0.75, 0.75
    rows[count - 1, count - 3:] = (-0.5, -2.0, 2.5)
    return rows


def dense_derivative(count):
    lower, upper = diagonals(count)
    matrix = np.eye(count) + np.diag(lower[1:], -1) + np.diag(upper[:-1], 1)
    return np.linalg.solve(matrix, stencil(count))


def x_tables(blocks, cells):
    count = blocks * cells
    lower, upper = diagonals(count)
    rows = stencil(count)
    down, pivot = np.zeros(count), np.ones(count)
    for i in range(1, count):
        down[i] = lower[i] / pivot[i - 1]
        pivot[i] = 1.0 - down[i] * upper[i - 1]
    up, pivot_up = np.zeros(count), np.ones(count)
    for i in range(count - 2, -1, -1):
        up[i] = upper[i] / pivot_up[i + 1]
        pivot_up[i] = 1.0 - up[i] * lower[i + 1]
    from_left = rows.copy()
    for i in range(1, count):
        from_left[i] -= down[i] * from_left[i - 1]
    from_right = rows.copy()
    for i in range(count - 2, -1, -1):
        from_right[i] -= up[i] * from_right[i + 1]
    weights = np.zeros((blocks, 2, cells))
    chain = np.zeros((blocks, 2))
    sweep = np.zeros((blocks, 3, cells))
    taps = np.zeros((blocks, 4, TAPS))
    ends = np.zeros((blocks, 4))
    for d in range(blocks):
        s, e = d * cells, (d + 1) * cells
        if d < blocks - 1:
            weights[d, 0] = from_left[e + 1, s:e]
            chain[d, 0] = np.prod(-down[s + 2:e + 2])
        if d > 0:
            weights[d, 1] = from_right[s - 2, s:e]
            chain[d, 1] = np.prod(-up[s - 2:e - 2])
        sweep[d, 0] = down[s:e]
        sweep[d, 1] = 1.0 / pivot[s:e]
        sweep[d, 2] = upper[s:e] / pivot[s:e]
        sweep[d, 1, -1] = 1.0 / (pivot[e - 1] + pivot_up[e - 1] - 1.0)
        taps[d, 0, 2:] = from_left[s, s:s + 3]
        taps[d, 3, :3] = from_right[e - 1, e - 3:e]
        for k in range(-2, 3):
            if 0 <= s + 1 + k:
                taps[d, 1, k + 2] = rows[s + 1, s + 1 + k]
            if e - 2 + k < count:
                taps[d, 2, k + 2] = rows[e - 2, e - 2 + k]
        ends[d, 0] = -1.0 / down[s + 1]
        ends[d, 2] = -1.0 / up[e - 2]
        if d > 0:
            ends[d, 1] = rows[s + 1, s - 1] / down[s + 1]
        if d < blocks - 1:
            ends[d, 3] = rows[e - 2, e] / up[e - 2]
    largest, hops, reach = np.abs(chain).max(), 1, np.abs(chain).max()
    while hops < blocks - 1 and reach >= np.finfo(np.float32).tiny:
        hops, reach = hops + 1, reach * largest
    edges = np.concatenate([taps.reshape(blocks, -1), ends], 1)
    return (
        weights.astype(np.float32),
        chain.astype(np.float32),
        sweep.astype(np.float32),
        edges.astype(np.float32),
        hops,
    )


def exchange_kernel(
    sizes, weights_ref, chain_ref, state_ref, flow_ref,
    left_sum, left_plane, right_sum, right_plane, low_ref, high_ref,
    field, to_right, to_left, on_right, on_left, far_left, far_right,
    load_sem, send_sem, recv_sem,
):
    blocks, groups = sizes
    _, cells, width, _ = field.shape
    block, group = lax.axis_index("gx"), lax.axis_index("yz")
    order = (0, 2, 4, 1, 3)
    crossing = (0, 2, 4)
    shifts = {"gx": (1, -1, 2, -2), "yz": (1, -1)}
    place = {"gx": (block, blocks), "yz": (group, groups)}

    def there(axis, shift):
        index, count = place[axis]
        return index + shift < count if shift > 0 else index + shift >= 0

    def other(axis, shift):
        index, count = place[axis]
        return {axis: jnp.clip(index + shift, 0, count - 1)}

    loads = {}
    for f in order:
        source = flow_ref if f == 4 else state_ref.at[f]
        loads[f] = pltpu.make_async_copy(source, field.at[f], load_sem.at[f])
        loads[f].start()

    barrier = pltpu.get_barrier_semaphore()
    pairs = [(axis, shift) for axis in shifts for shift in shifts[axis]]
    for axis, shift in pairs:
        @pl.when(there(axis, shift))
        def _():
            pl.semaphore_signal(
                barrier, inc=1, device_id=other(axis, shift),
                device_id_type=pl.DeviceIdType.MESH,
            )
    present = [there(axis, shift).astype(jnp.int32) for axis, shift in pairs]
    pl.semaphore_wait(barrier, sum(present[1:], present[0]))

    sent = []

    def copy(kind, f, source, target, axis, shift):
        moved = pltpu.make_async_remote_copy(
            src_ref=source, dst_ref=target,
            send_sem=send_sem.at[kind, f], recv_sem=recv_sem.at[kind, f],
            device_id=other(axis, shift), device_id_type=pl.DeviceIdType.MESH,
        )
        sent.append((moved, axis, shift))

        @pl.when(there(axis, shift))
        def _():
            moved.start()

        return moved, axis, shift

    def arrive(entry, targets):
        moved, axis, shift = entry

        @pl.when(there(axis, -shift))
        def _():
            moved.wait_recv()

        @pl.when(jnp.logical_not(there(axis, -shift)))
        def _():
            targets[...] = jnp.zeros_like(targets)

    near, rest = {}, []
    for f in order:
        loads[f].wait()
        plane_r = copy(0, f, field.at[f, cells - 1], left_plane.at[f], "gx", 1)
        plane_l = copy(1, f, field.at[f, 0], right_plane.at[f], "gx", -1)
        rest += [(plane_r, left_plane.at[f]), (plane_l, right_plane.at[f])]
        if f in crossing:
            slot = crossing.index(f)
            rest.append((copy(
                2, f, field.at[f, :, width - TILE:width], low_ref.at[slot], "yz", 1
            ), low_ref.at[slot]))
            rest.append((copy(
                3, f, field.at[f, :, 0:TILE], high_ref.at[slot], "yz", -1
            ), high_ref.at[slot]))
        for j in range(0, width, TILE):
            total_right = weights_ref[0, 0] * field[f, 0, j:j + TILE]
            total_left = weights_ref[1, 0] * field[f, 0, j:j + TILE]
            for i in range(1, cells):
                value = field[f, i, j:j + TILE]
                total_right += weights_ref[0, i] * value
                total_left += weights_ref[1, i] * value
            to_right[f, j:j + TILE] = total_right
            to_left[f, j:j + TILE] = total_left
        near[f] = (
            copy(4, f, to_right.at[f], left_sum.at[f], "gx", 1),
            copy(5, f, to_left.at[f], right_sum.at[f], "gx", -1),
        )
    far = {}
    for f in order:
        arrive(near[f][0], left_sum.at[f])
        arrive(near[f][1], right_sum.at[f])
        on_right[f] = to_right[f] + chain_ref[0, 0] * left_sum[f]
        on_left[f] = to_left[f] + chain_ref[0, 1] * right_sum[f]
        far[f] = (
            copy(6, f, on_right.at[f], far_left.at[f], "gx", 2),
            copy(7, f, on_left.at[f], far_right.at[f], "gx", -2),
        )
    for f in order:
        arrive(far[f][0], far_left.at[f])
        arrive(far[f][1], far_right.at[f])
    for entry, targets in rest:
        arrive(entry, targets)
    for moved, axis, shift in sent:
        @pl.when(there(axis, shift))
        def _():
            moved.wait_send()
    for f in order:
        left_sum[f] = left_sum[f] + chain_ref[0, 2] * far_left[f]
        right_sum[f] = right_sum[f] + chain_ref[0, 3] * far_right[f]


def signal_kernel(groups, count, piece_ref, out_ref, landing, send_sem, recv_sem):
    me = lax.axis_index("gx") * groups + lax.axis_index("yz")

    def partner(k):
        index = lax.rem(me + k, count)
        return {"gx": lax.div(index, groups), "yz": lax.rem(index, groups)}, index

    barrier = pltpu.get_barrier_semaphore()
    for k in range(1, count):
        pl.semaphore_signal(
            barrier, inc=1, device_id=partner(k)[0], device_id_type=pl.DeviceIdType.MESH
        )
    pl.semaphore_wait(barrier, count - 1)
    copies = []
    for k in range(1, count):
        target, index = partner(k)
        copies.append(pltpu.make_async_remote_copy(
            src_ref=piece_ref.at[index], dst_ref=landing.at[k - 1],
            send_sem=send_sem.at[k - 1], recv_sem=recv_sem.at[k - 1],
            device_id=target, device_id_type=pl.DeviceIdType.MESH,
        ))
        copies[-1].start()
    for moved in copies:
        moved.wait()
    total = piece_ref[me]
    for k in range(count - 1):
        total += landing[k]
    out_ref[...] = total


def main_kernel(
    cells, width, depth,
    row_ref, sweep_ref, edges_ref,
    state_ref, flow_ref, left_sum, left_plane, right_sum, right_plane, low_ref, high_ref,
    zhi_ref, zlo_ref, along_z_ref, normal_ref, pos_ref, observer_ref, bin_ref,
    next_ref, signal_ref,
    wide, swept, zrate, rate, picked,
):
    step = pl.program_id(0)
    rows = pl.ds(pl.multiple_of(step * TILE, TILE), TILE)
    window = pl.ds(pl.multiple_of(step * TILE, TILE), 3 * TILE)

    def load(f, i):
        return flow_ref[i, rows, :] if f == 4 else state_ref[f, i, rows, :]

    @pl.when(step == 0)
    def _():
        def widen(i, carry):
            for slot, f in enumerate((0, 2, 4)):
                body = flow_ref[i] if f == 4 else state_ref[f, i]
                wide[slot, i, TILE:TILE + width, :] = body
                wide[slot, i, 0:TILE, :] = low_ref[slot, i]
                wide[slot, i, TILE + width:2 * TILE + width, :] = high_ref[slot, i]
            return carry
        lax.fori_loop(0, cells, widen, 0)

    for slot, f in enumerate((0, 3, 4)):
        block = flow_ref[:, rows, :] if f == 4 else state_ref[f, :, rows, :]
        block = block.reshape(cells * TILE, depth)
        high = block.astype(jnp.bfloat16)
        rest = (block - high.astype(jnp.float32)).astype(jnp.bfloat16)
        out = jnp.dot(rest, zhi_ref[...], preferred_element_type=jnp.float32)
        out += jnp.dot(high, zlo_ref[...], preferred_element_type=jnp.float32)
        out += jnp.dot(high, zhi_ref[...], preferred_element_type=jnp.float32)
        zrate[slot] = out.reshape(cells, TILE, depth)

    fields = range(5)

    def tap(k, position):
        return edges_ref[0, k * TAPS + position + 2]

    def end(k):
        return edges_ref[0, 4 * TAPS + k]

    carry = []
    for f in fields:
        first = tap(0, 0) * load(f, 0) + tap(0, 1) * load(f, 1) + tap(0, 2) * load(f, 2)
        value = first + end(0) * left_sum[f] + end(1) * left_plane[f]
        swept[f, 0] = value
        second = (
            tap(1, -1) * load(f, 0) + tap(1, 0) * load(f, 1)
            + tap(1, 1) * load(f, 2) + tap(1, 2) * load(f, 3) + tap(1, -2) * left_plane[f]
        )
        value = second - sweep_ref[0, 1] * value
        swept[f, 1] = value
        carry.append(value)

    def forward(i, carry):
        new = []
        factor = sweep_ref[0, i]
        for f in fields:
            rhs = 7.0 / 9.0 * (load(f, i + 1) - load(f, i - 1)) + 1.0 / 36.0 * (
                load(f, i + 2) - load(f, i - 2)
            )
            value = rhs - factor * carry[f]
            swept[f, i] = value
            new.append(value)
        return tuple(new)

    carry = lax.fori_loop(2, cells - 2, forward, tuple(carry), unroll=2)
    solved = []
    n = cells
    for f in fields:
        before = (
            tap(2, -2) * load(f, n - 4) + tap(2, -1) * load(f, n - 3) + tap(2, 0) * load(f, n - 2)
            + tap(2, 1) * load(f, n - 1) + tap(2, 2) * right_plane[f]
        )
        value = before - sweep_ref[0, n - 2] * carry[f]
        swept[f, n - 2] = value
        last = (
            tap(3, -2) * load(f, n - 3) + tap(3, -1) * load(f, n - 2) + tap(3, 0) * load(f, n - 1)
            + end(2) * right_sum[f] + end(3) * right_plane[f]
        )
        solved.append((last - sweep_ref[0, n - 1] * value) * sweep_ref[1, n - 1])

    def y_rate(slot, i):
        whole = wide[slot, i, window, :]

        def take(shift):
            return whole[TILE + shift:2 * TILE + shift]

        return (
            0.75 * (take(1) - take(-1))
            - 0.15 * (take(2) - take(-2))
            + 1.0 / 60.0 * (take(3) - take(-3))
        )

    def finish(i, x):
        p, u, v, w, flow = (load(f, i) for f in fields)
        rates = (
            -(flow * x[0] + x[1] + y_rate(1, i) + zrate[1, i]),
            -(flow * x[1] + u * x[4] + v * y_rate(2, i) + w * zrate[2, i] + x[0]),
            -(flow * x[2] + y_rate(0, i)),
            -(flow * x[3] + zrate[0, i]),
        )
        place = pl.ds(pl.multiple_of(i * width + step * TILE, TILE), TILE)
        for c, old in enumerate((p, u, v, w)):
            rate[c, place, :] = rates[c]
            new = old + time_step * rates[c]
            next_ref[c, i] = new
            if c == 0:
                rate[4, place, :] = new

    finish(n - 1, solved)

    def backward(k, carry):
        i = n - 2 - k
        x = tuple(
            swept[f, i] * sweep_ref[1, i] - sweep_ref[2, i] * carry[f] for f in fields
        )
        finish(i, x)
        return x

    lax.fori_loop(0, n - 1, backward, tuple(solved))

    @pl.when(step == pl.num_programs(0) - 1)
    def _():
        faces = picked.shape[1]

        def pick(k, carry):
            row = row_ref[0, k]
            for c in range(5):
                picked[c, pl.ds(k, 1), :] = rate[c, pl.ds(row, 1), :]
            return carry

        lax.fori_loop(0, faces, pick, 0, unroll=4)
        mask = lax.broadcasted_iota(jnp.int32, (faces, depth), 1) == along_z_ref[...]
        at = [
            jnp.sum(jnp.where(mask, picked[c], 0.0), axis=1, keepdims=True) for c in range(5)
        ]
        normal = [normal_ref[:, c:c + 1] for c in range(3)]
        normal_rate = normal[0] * at[1] + normal[1] * at[2] + normal[2] * at[3]
        offset = [observer_ref[c:c + 1, :] - pos_ref[:, c:c + 1] for c in range(3)]
        distance = jnp.sqrt(
            offset[0] * offset[0] + offset[1] * offset[1] + offset[2] * offset[2]
        )
        normal_r = (
            normal[0] * offset[0] + normal[1] * offset[1] + normal[2] * offset[2]
        ) / distance
        contribution = (normal_rate + (at[0] + at[4] / distance) * normal_r) / (
            four_pi * distance
        )
        bins = bin_ref[...]

        def gather(b, carry):
            signal_ref[pl.ds(b, 1), :] = jnp.sum(
                jnp.where(bins == b, contribution, 0.0), axis=0, keepdims=True
            )
            return carry

        lax.fori_loop(0, BINS, gather, 0, unroll=2)


def per_device(sizes, state, mean_flow, face_cell, face_normal, face_pos, observer_pos, time_bin):
    blocks, groups = sizes
    _, cells, width, depth = state.shape
    faces, observers = time_bin.shape
    tiles = width // TILE
    block, group = lax.axis_index("gx"), lax.axis_index("yz")
    weights, chain, sweep, edges, hops = x_tables(blocks, cells)

    def mine(table):
        return lax.dynamic_index_in_dim(jnp.asarray(table), block, 0, keepdims=False)

    params = dict(vmem_limit_bytes=60 * 1024 * 1024)
    assert hops <= 3
    links = np.zeros((blocks, 1, 4), np.float32)
    links[:, 0, :2] = chain
    links[1:, 0, 2] = chain[:-1, 0]
    links[:-1, 0, 3] = chain[1:, 1]
    plane = jax.ShapeDtypeStruct((5, width, depth), jnp.float32)
    edge = jax.ShapeDtypeStruct((3, cells, TILE, depth), jnp.float32)
    plane_spec = pl.BlockSpec((5, TILE, depth), lambda j: (0, j, 0))
    scratch_plane = VMEM((5, width, depth), jnp.float32)
    received = pl.pallas_call(
        functools.partial(exchange_kernel, sizes),
        out_shape=(plane,) * 4 + (edge,) * 2,
        in_specs=[
            pl.BlockSpec(memory_space=SMEM),
            pl.BlockSpec(memory_space=SMEM),
            pl.BlockSpec(memory_space=pl.ANY),
            pl.BlockSpec(memory_space=pl.ANY),
        ],
        out_specs=(pl.BlockSpec(memory_space=VMEM),) * 6,
        scratch_shapes=[VMEM((5, cells, width, depth), jnp.float32)]
        + [scratch_plane] * 6
        + [
            pltpu.SemaphoreType.DMA((5,)),
            pltpu.SemaphoreType.DMA((8, 5)),
            pltpu.SemaphoreType.DMA((8, 5)),
        ],
        compiler_params=pltpu.CompilerParams(
            collective_id=0, has_side_effects=True, vmem_limit_bytes=40 * 1024 * 1024
        ),
    )(mine(weights), mine(links), state, mean_flow)

    operator = dense_derivative(depth).T.astype(np.float32)
    z_high = jnp.asarray(operator).astype(jnp.bfloat16)
    z_low = (jnp.asarray(operator) - z_high.astype(jnp.float32)).astype(jnp.bfloat16)

    planes = width * groups
    along_x = face_cell // (planes * depth) - block * cells
    along_y = face_cell // depth % planes - group * width
    along_z = face_cell % depth
    row = (along_x * width + along_y).reshape(1, faces)

    def whole(*shape):
        return pl.BlockSpec(shape, lambda j: (0,) * len(shape))

    smem = pl.BlockSpec(memory_space=SMEM)
    state_next, signal = pl.pallas_call(
        functools.partial(main_kernel, cells, width, depth),
        grid=(tiles,),
        out_shape=(
            jax.ShapeDtypeStruct(state.shape, jnp.float32),
            jax.ShapeDtypeStruct((BINS, observers), jnp.float32),
        ),
        in_specs=[
            smem, smem, smem,
            whole(4, cells, width, depth), whole(cells, width, depth),
            plane_spec, plane_spec, plane_spec, plane_spec,
            whole(3, cells, TILE, depth), whole(3, cells, TILE, depth),
            whole(depth, depth), whole(depth, depth),
            whole(faces, 1), whole(faces, 3), whole(faces, 3),
            whole(3, observers), whole(faces, observers),
        ],
        out_specs=(
            pl.BlockSpec((4, cells, TILE, depth), lambda j: (0, 0, j, 0)),
            whole(BINS, observers),
        ),
        scratch_shapes=[
            VMEM((3, cells, width + 2 * TILE, depth), jnp.float32),
            VMEM((5, cells, TILE, depth), jnp.float32),
            VMEM((3, cells, TILE, depth), jnp.float32),
            VMEM((5, cells * width, depth), jnp.float32),
            VMEM((5, faces, depth), jnp.float32),
        ],
        compiler_params=pltpu.CompilerParams(**params),
    )(
        row, mine(sweep), mine(edges.reshape(blocks, 1, -1)),
        state, mean_flow, *received,
        z_high, z_low, along_z.reshape(faces, 1), face_normal.T, face_pos.T,
        observer_pos, time_bin,
    )
    devices = blocks * groups
    share = observers // devices
    signal = pl.pallas_call(
        functools.partial(signal_kernel, groups, devices),
        out_shape=jax.ShapeDtypeStruct((share, BINS), jnp.float32),
        in_specs=[pl.BlockSpec(memory_space=VMEM)],
        out_specs=pl.BlockSpec(memory_space=VMEM),
        scratch_shapes=[
            VMEM((devices - 1, share, BINS), jnp.float32),
            pltpu.SemaphoreType.DMA((devices - 1,)),
            pltpu.SemaphoreType.DMA((devices - 1,)),
        ],
        compiler_params=pltpu.CompilerParams(collective_id=1, has_side_effects=True),
    )(signal.T.reshape(devices, share, BINS))
    return state_next, signal


def solution(mesh):
    in_specs = (
        P(None, "gx", "yz", None),
        P("gx", "yz", None),
        P(("gx", "yz")),
        P(None, ("gx", "yz")),
        P(None, ("gx", "yz")),
        P(),
        P(("gx", "yz"), None),
    )
    out_specs = (P(None, "gx", "yz", None), P(("gx", "yz"), None))
    sizes = (mesh.shape["gx"], mesh.shape["yz"])
    return jax.shard_map(
        functools.partial(per_device, sizes),
        mesh=mesh, in_specs=in_specs, out_specs=out_specs, check_vma=False,
    )
```

```python
import functools

import numpy as np
import jax
import jax.numpy as jnp
from jax import lax
from jax.experimental import pallas as pl
from jax.experimental.pallas import tpu as pltpu
from jax.sharding import PartitionSpec as P

BINS = 64
TILE = 8
TAPS = 5

time_step = 0.25
four_pi = 4.0 * 3.141592653589793
VMEM = pltpu.VMEM
SMEM = pltpu.SMEM


def diagonals(count):
    lower = np.full(count, 1.0 / 3.0)
    upper = np.full(count, 1.0 / 3.0)
    lower[1] = lower[count - 2] = upper[1] = upper[count - 2] = 0.25
    lower[0] = upper[count - 1] = 0.0
    lower[count - 1] = upper[0] = 2.0
    return lower, upper


def stencil(count):
    rows = np.zeros((count, count))
    for i in range(2, count - 2):
        rows[i, i + 1], rows[i, i - 1] = 7.0 / 9.0, -7.0 / 9.0
        rows[i, i + 2], rows[i, i - 2] = 1.0 / 36.0, -1.0 / 36.0
    rows[0, :3] = (-2.5, 2.0, 0.5)
    rows[1, 0], rows[1, 2] = -0.75, 0.75
    rows[count - 2, count - 3], rows[count - 2, count - 1] = -0.75, 0.75
    rows[count - 1, count - 3:] = (-0.5, -2.0, 2.5)
    return rows


def dense_derivative(count):
    lower, upper = diagonals(count)
    matrix = np.eye(count) + np.diag(lower[1:], -1) + np.diag(upper[:-1], 1)
    return np.linalg.solve(matrix, stencil(count))


def x_tables(blocks, cells):
    count = blocks * cells
    lower, upper = diagonals(count)
    rows = stencil(count)
    down, pivot = np.zeros(count), np.ones(count)
    for i in range(1, count):
        down[i] = lower[i] / pivot[i - 1]
        pivot[i] = 1.0 - down[i] * upper[i - 1]
    up, pivot_up = np.zeros(count), np.ones(count)
    for i in range(count - 2, -1, -1):
        up[i] = upper[i] / pivot_up[i + 1]
        pivot_up[i] = 1.0 - up[i] * lower[i + 1]
    from_left = rows.copy()
    for i in range(1, count):
        from_left[i] -= down[i] * from_left[i - 1]
    from_right = rows.copy()
    for i in range(count - 2, -1, -1):
        from_right[i] -= up[i] * from_right[i + 1]
    weights = np.zeros((blocks, 2, cells))
    chain = np.zeros((blocks, 2))
    sweep = np.zeros((blocks, 3, cells))
    taps = np.zeros((blocks, 4, TAPS))
    ends = np.zeros((blocks, 4))
    for d in range(blocks):
        s, e = d * cells, (d + 1) * cells
        if d < blocks - 1:
            weights[d, 0] = from_left[e + 1, s:e]
            chain[d, 0] = np.prod(-down[s + 2:e + 2])
        if d > 0:
            weights[d, 1] = from_right[s - 2, s:e]
            chain[d, 1] = np.prod(-up[s - 2:e - 2])
        sweep[d, 0] = down[s:e]
        sweep[d, 1] = 1.0 / pivot[s:e]
        sweep[d, 2] = upper[s:e] / pivot[s:e]
        sweep[d, 1, -1] = 1.0 / (pivot[e - 1] + pivot_up[e - 1] - 1.0)
        taps[d, 0, 2:] = from_left[s, s:s + 3]
        taps[d, 3, :3] = from_right[e - 1, e - 3:e]
        for k in range(-2, 3):
            if 0 <= s + 1 + k:
                taps[d, 1, k + 2] = rows[s + 1, s + 1 + k]
            if e - 2 + k < count:
                taps[d, 2, k + 2] = rows[e - 2, e - 2 + k]
        ends[d, 0] = -1.0 / down[s + 1]
        ends[d, 2] = -1.0 / up[e - 2]
        if d > 0:
            ends[d, 1] = rows[s + 1, s - 1] / down[s + 1]
        if d < blocks - 1:
            ends[d, 3] = rows[e - 2, e] / up[e - 2]
    largest, hops, reach = np.abs(chain).max(), 1, np.abs(chain).max()
    while hops < blocks - 1 and reach >= np.finfo(np.float32).tiny:
        hops, reach = hops + 1, reach * largest
    edges = np.concatenate([taps.reshape(blocks, -1), ends], 1)
    return (
        weights.astype(np.float32),
        chain.astype(np.float32),
        sweep.astype(np.float32),
        edges.astype(np.float32),
        hops,
    )


def exchange_kernel(
    sizes, table_ref, state_ref, flow_ref, zhi_ref, zlo_ref,
    left_sum, left_plane, right_sum, right_plane, low_ref, high_ref, z_out,
    zrate, field, to_right, to_left, on_right, on_left, far_left, far_right,
    load_sem, store_sem, send_sem, recv_sem,
):
    blocks, groups = sizes
    _, cells, width, _ = field.shape
    block, group = lax.axis_index("gx"), lax.axis_index("yz")
    order = (0, 2, 4, 1, 3)
    crossing = (0, 2, 4)

    def weight(side, i):
        return table_ref[0, side * cells + i]

    shifts = {"gx": (1, -1, 2, -2), "yz": (1, -1)}
    place = {"gx": (block, blocks), "yz": (group, groups)}

    def there(axis, shift):
        index, count = place[axis]
        return index + shift < count if shift > 0 else index + shift >= 0

    def other(axis, shift):
        index, count = place[axis]
        return {axis: jnp.clip(index + shift, 0, count - 1)}

    loads = {}
    for f in order:
        source = flow_ref if f == 4 else state_ref.at[f]
        loads[f] = pltpu.make_async_copy(source, field.at[f], load_sem.at[f])
        loads[f].start()

    barrier = pltpu.get_barrier_semaphore()
    pairs = [(axis, shift) for axis in shifts for shift in shifts[axis]]
    for axis, shift in pairs:
        @pl.when(there(axis, shift))
        def _():
            pl.semaphore_signal(
                barrier, inc=1, device_id=other(axis, shift),
                device_id_type=pl.DeviceIdType.MESH,
            )
    present = [there(axis, shift).astype(jnp.int32) for axis, shift in pairs]
    pl.semaphore_wait(barrier, sum(present[1:], present[0]))

    sent = []

    def copy(kind, f, source, target, axis, shift):
        moved = pltpu.make_async_remote_copy(
            src_ref=source, dst_ref=target,
            send_sem=send_sem.at[kind, f], recv_sem=recv_sem.at[kind, f],
            device_id=other(axis, shift), device_id_type=pl.DeviceIdType.MESH,
        )
        sent.append((moved, axis, shift))

        @pl.when(there(axis, shift))
        def _():
            moved.start()

        return moved, axis, shift

    def arrive(entry, targets):
        moved, axis, shift = entry

        @pl.when(there(axis, -shift))
        def _():
            moved.wait_recv()

        @pl.when(jnp.logical_not(there(axis, -shift)))
        def _():
            targets[...] = jnp.zeros_like(targets)

    near, rest = {}, []
    for f in order:
        loads[f].wait()
        plane_r = copy(0, f, field.at[f, cells - 1], left_plane.at[f], "gx", 1)
        plane_l = copy(1, f, field.at[f, 0], right_plane.at[f], "gx", -1)
        rest += [(plane_r, left_plane.at[f]), (plane_l, right_plane.at[f])]
        if f in crossing:
            slot = crossing.index(f)
            rest.append((copy(
                2, f, field.at[f, :, width - TILE:width], low_ref.at[slot], "yz", 1
            ), low_ref.at[slot]))
            rest.append((copy(
                3, f, field.at[f, :, 0:TILE], high_ref.at[slot], "yz", -1
            ), high_ref.at[slot]))
        for j in range(0, width, TILE):
            total_right = weight(0, 0) * field[f, 0, j:j + TILE]
            total_left = weight(1, 0) * field[f, 0, j:j + TILE]
            for i in range(1, cells):
                value = field[f, i, j:j + TILE]
                total_right += weight(0, i) * value
                total_left += weight(1, i) * value
            to_right[f, j:j + TILE] = total_right
            to_left[f, j:j + TILE] = total_left
        near[f] = (
            copy(4, f, to_right.at[f], left_sum.at[f], "gx", 1),
            copy(5, f, to_left.at[f], right_sum.at[f], "gx", -1),
        )
    stores = []
    group_of = 4 if cells % 4 == 0 else 1
    for slot, f in enumerate((0, 3, 4)):
        def multiply(k, carry, slot=slot, f=f):
            planes = pl.ds(k * group_of, group_of)
            block = field[f, planes].reshape(group_of * width, -1)
            high = block.astype(jnp.bfloat16)
            rest = (block - high.astype(jnp.float32)).astype(jnp.bfloat16)
            out = jnp.dot(rest, zhi_ref[...], preferred_element_type=jnp.float32)
            out += jnp.dot(high, zlo_ref[...], preferred_element_type=jnp.float32)
            out += jnp.dot(high, zhi_ref[...], preferred_element_type=jnp.float32)
            zrate[slot, planes] = out.reshape(group_of, width, -1)
            return carry
        lax.fori_loop(0, cells // group_of, multiply, 0)
        stores.append(pltpu.make_async_copy(
            zrate.at[slot], z_out.at[slot], store_sem.at[slot]
        ))
        stores[-1].start()
    far = {}
    for f in order:
        arrive(near[f][0], left_sum.at[f])
        arrive(near[f][1], right_sum.at[f])
        on_right[f] = to_right[f] + table_ref[0, 5 * cells + 0] * left_sum[f]
        on_left[f] = to_left[f] + table_ref[0, 5 * cells + 1] * right_sum[f]
        far[f] = (
            copy(6, f, on_right.at[f], far_left.at[f], "gx", 2),
            copy(7, f, on_left.at[f], far_right.at[f], "gx", -2),
        )
    for f in order:
        arrive(far[f][0], far_left.at[f])
        arrive(far[f][1], far_right.at[f])
    for entry, targets in rest:
        arrive(entry, targets)
    for store in stores:
        store.wait()
    for moved, axis, shift in sent:
        @pl.when(there(axis, shift))
        def _():
            moved.wait_send()
    for f in order:
        left_sum[f] = left_sum[f] + table_ref[0, 5 * cells + 2] * far_left[f]
        right_sum[f] = right_sum[f] + table_ref[0, 5 * cells + 3] * far_right[f]


def signal_kernel(groups, count, piece_ref, out_ref, landing, send_sem, recv_sem):
    me = lax.axis_index("gx") * groups + lax.axis_index("yz")

    def partner(k):
        index = lax.rem(me + k, count)
        return {"gx": lax.div(index, groups), "yz": lax.rem(index, groups)}, index

    barrier = pltpu.get_barrier_semaphore()
    for k in range(1, count):
        pl.semaphore_signal(
            barrier, inc=1, device_id=partner(k)[0], device_id_type=pl.DeviceIdType.MESH
        )
    pl.semaphore_wait(barrier, count - 1)
    copies = []
    for k in range(1, count):
        target, index = partner(k)
        copies.append(pltpu.make_async_remote_copy(
            src_ref=piece_ref.at[index], dst_ref=landing.at[k - 1],
            send_sem=send_sem.at[k - 1], recv_sem=recv_sem.at[k - 1],
            device_id=target, device_id_type=pl.DeviceIdType.MESH,
        ))
        copies[-1].start()
    for moved in copies:
        moved.wait()
    total = piece_ref[me]
    for k in range(count - 1):
        total += landing[k]
    out_ref[...] = total


def main_kernel(
    cells, width, depth,
    row_ref, table_ref,
    state_ref, flow_ref, left_sum, left_plane, right_sum, right_plane, low_ref, high_ref,
    zrate, geometry_ref, observer_ref, bin_ref,
    next_ref, signal_ref,
    wide, swept, rate, picked,
):
    step = pl.program_id(0)
    rows = pl.ds(pl.multiple_of(step * TILE, TILE), TILE)
    window = pl.ds(pl.multiple_of(step * TILE, TILE), 3 * TILE)

    def load(f, i):
        return flow_ref[i, rows, :] if f == 4 else state_ref[f, i, rows, :]

    @pl.when(step == 0)
    def _():
        def widen(i, carry):
            for slot, f in enumerate((0, 2, 4)):
                body = flow_ref[i] if f == 4 else state_ref[f, i]
                wide[slot, i, TILE:TILE + width, :] = body
                wide[slot, i, 0:TILE, :] = low_ref[slot, i]
                wide[slot, i, TILE + width:2 * TILE + width, :] = high_ref[slot, i]
            return carry
        lax.fori_loop(0, cells, widen, 0)

    fields = range(5)

    def tap(k, position):
        return table_ref[0, 5 * cells + 4 + k * TAPS + position + 2]

    def end(k):
        return table_ref[0, 5 * cells + 4 + 4 * TAPS + k]

    def sweep(k, i):
        return table_ref[0, (2 + k) * cells + i]

    carry = []
    for f in fields:
        first = tap(0, 0) * load(f, 0) + tap(0, 1) * load(f, 1) + tap(0, 2) * load(f, 2)
        value = first + end(0) * left_sum[f] + end(1) * left_plane[f]
        swept[f, 0] = value
        second = (
            tap(1, -1) * load(f, 0) + tap(1, 0) * load(f, 1)
            + tap(1, 1) * load(f, 2) + tap(1, 2) * load(f, 3) + tap(1, -2) * left_plane[f]
        )
        value = second - sweep(0, 1) * value
        swept[f, 1] = value
        carry.append(value)

    def forward(i, carry):
        new = []
        factor = sweep(0, i)
        for f in fields:
            rhs = 7.0 / 9.0 * (load(f, i + 1) - load(f, i - 1)) + 1.0 / 36.0 * (
                load(f, i + 2) - load(f, i - 2)
            )
            value = rhs - factor * carry[f]
            swept[f, i] = value
            new.append(value)
        return tuple(new)

    carry = lax.fori_loop(2, cells - 2, forward, tuple(carry), unroll=2)
    solved = []
    n = cells
    for f in fields:
        before = (
            tap(2, -2) * load(f, n - 4) + tap(2, -1) * load(f, n - 3) + tap(2, 0) * load(f, n - 2)
            + tap(2, 1) * load(f, n - 1) + tap(2, 2) * right_plane[f]
        )
        value = before - sweep(0, n - 2) * carry[f]
        swept[f, n - 2] = value
        last = (
            tap(3, -2) * load(f, n - 3) + tap(3, -1) * load(f, n - 2) + tap(3, 0) * load(f, n - 1)
            + end(2) * right_sum[f] + end(3) * right_plane[f]
        )
        solved.append((last - sweep(0, n - 1) * value) * sweep(1, n - 1))

    def y_rate(slot, i):
        whole = wide[slot, i, window, :]

        def take(shift):
            return whole[TILE + shift:2 * TILE + shift]

        return (
            0.75 * (take(1) - take(-1))
            - 0.15 * (take(2) - take(-2))
            + 1.0 / 60.0 * (take(3) - take(-3))
        )

    def finish(i, x):
        p, u, v, w, flow = (load(f, i) for f in fields)
        rates = (
            -(flow * x[0] + x[1] + y_rate(1, i) + zrate[1, i]),
            -(flow * x[1] + u * x[4] + v * y_rate(2, i) + w * zrate[2, i] + x[0]),
            -(flow * x[2] + y_rate(0, i)),
            -(flow * x[3] + zrate[0, i]),
        )
        place = pl.ds(pl.multiple_of(i * width + step * TILE, TILE), TILE)
        for c, old in enumerate((p, u, v, w)):
            rate[c, place, :] = rates[c]
            new = old + time_step * rates[c]
            next_ref[c, i] = new
            if c == 0:
                rate[4, place, :] = new

    finish(n - 1, solved)

    def backward(k, carry):
        i = n - 2 - k
        x = tuple(
            swept[f, i] * sweep(1, i) - sweep(2, i) * carry[f] for f in fields
        )
        finish(i, x)
        return x

    lax.fori_loop(0, n - 1, backward, tuple(solved))

    @pl.when(step == pl.num_programs(0) - 1)
    def _():
        faces = picked.shape[1]

        def pick(k, carry):
            row = row_ref[0, k]
            for c in range(5):
                picked[c, pl.ds(k, 1), :] = rate[c, pl.ds(row, 1), :]
            return carry

        lax.fori_loop(0, faces, pick, 0, unroll=4)
        mask = lax.broadcasted_iota(jnp.int32, (faces, depth), 1) == geometry_ref[:, 6:7].astype(jnp.int32)
        at = [
            jnp.sum(jnp.where(mask, picked[c], 0.0), axis=1, keepdims=True) for c in range(5)
        ]
        normal = [geometry_ref[:, c:c + 1] for c in range(3)]
        normal_rate = normal[0] * at[1] + normal[1] * at[2] + normal[2] * at[3]
        offset = [observer_ref[c:c + 1, :] - geometry_ref[:, 3 + c:4 + c] for c in range(3)]
        distance = jnp.sqrt(
            offset[0] * offset[0] + offset[1] * offset[1] + offset[2] * offset[2]
        )
        normal_r = (
            normal[0] * offset[0] + normal[1] * offset[1] + normal[2] * offset[2]
        ) / distance
        contribution = (normal_rate + (at[0] + at[4] / distance) * normal_r) / (
            four_pi * distance
        )
        bins = bin_ref[...]

        def gather(b, carry):
            signal_ref[pl.ds(b, 1), :] = jnp.sum(
                jnp.where(bins == b, contribution, 0.0), axis=0, keepdims=True
            )
            return carry

        lax.fori_loop(0, BINS, gather, 0, unroll=2)


def per_device(sizes, state, mean_flow, face_cell, face_normal, face_pos, observer_pos, time_bin):
    blocks, groups = sizes
    _, cells, width, depth = state.shape
    faces, observers = time_bin.shape
    tiles = width // TILE
    block, group = lax.axis_index("gx"), lax.axis_index("yz")
    weights, chain, sweep, edges, hops = x_tables(blocks, cells)

    params = dict(vmem_limit_bytes=60 * 1024 * 1024)
    assert hops <= 3
    links = np.zeros((blocks, 1, 4), np.float32)
    links[:, 0, :2] = chain
    links[1:, 0, 2] = chain[:-1, 0]
    links[:-1, 0, 3] = chain[1:, 1]
    tables = np.concatenate(
        [part.reshape(blocks, 1, -1) for part in (weights, sweep, links, edges)], axis=2
    )
    table = lax.dynamic_index_in_dim(jnp.asarray(tables), block, 0, keepdims=False)
    plane = jax.ShapeDtypeStruct((5, width, depth), jnp.float32)
    edge = jax.ShapeDtypeStruct((3, cells, TILE, depth), jnp.float32)
    plane_spec = pl.BlockSpec((5, TILE, depth), lambda j: (0, j, 0))
    scratch_plane = VMEM((5, width, depth), jnp.float32)
    operator = dense_derivative(depth).T.astype(np.float32)
    z_high = jnp.asarray(operator).astype(jnp.bfloat16)
    z_low = (jnp.asarray(operator) - z_high.astype(jnp.float32)).astype(jnp.bfloat16)

    *received, z_rates = pl.pallas_call(
        functools.partial(exchange_kernel, sizes),
        out_shape=(plane,) * 4 + (edge,) * 2
        + (jax.ShapeDtypeStruct((3, cells, width, depth), jnp.float32),),
        in_specs=[
            pl.BlockSpec(memory_space=SMEM),
            pl.BlockSpec(memory_space=pl.ANY),
            pl.BlockSpec(memory_space=pl.ANY),
            pl.BlockSpec(memory_space=VMEM),
            pl.BlockSpec(memory_space=VMEM),
        ],
        out_specs=(pl.BlockSpec(memory_space=VMEM),) * 6 + (pl.BlockSpec(memory_space=pl.ANY),),
        scratch_shapes=[VMEM((3, cells, width, depth), jnp.float32)]
        + [VMEM((5, cells, width, depth), jnp.float32)]
        + [scratch_plane] * 6
        + [
            pltpu.SemaphoreType.DMA((5,)),
            pltpu.SemaphoreType.DMA((3,)),
            pltpu.SemaphoreType.DMA((8, 5)),
            pltpu.SemaphoreType.DMA((8, 5)),
        ],
        compiler_params=pltpu.CompilerParams(
            collective_id=0, has_side_effects=True, vmem_limit_bytes=60 * 1024 * 1024
        ),
    )(table, state, mean_flow, z_high, z_low)

    planes = width * groups
    along_x = face_cell // (planes * depth) - block * cells
    along_y = face_cell // depth % planes - group * width
    along_z = face_cell % depth
    row = (along_x * width + along_y).reshape(1, faces)

    geometry = jnp.concatenate(
        [face_normal, face_pos, along_z.astype(jnp.float32)[None]]
    ).T

    def whole(*shape):
        return pl.BlockSpec(shape, lambda j: (0,) * len(shape))

    smem = pl.BlockSpec(memory_space=SMEM)
    state_next, signal = pl.pallas_call(
        functools.partial(main_kernel, cells, width, depth),
        grid=(tiles,),
        out_shape=(
            jax.ShapeDtypeStruct(state.shape, jnp.float32),
            jax.ShapeDtypeStruct((BINS, observers), jnp.float32),
        ),
        in_specs=[
            smem, smem,
            whole(4, cells, width, depth), whole(cells, width, depth),
            plane_spec, plane_spec, plane_spec, plane_spec,
            whole(3, cells, TILE, depth), whole(3, cells, TILE, depth),
            pl.BlockSpec((3, cells, TILE, depth), lambda j: (0, 0, j, 0)),
            whole(faces, 7),
            whole(3, observers), whole(faces, observers),
        ],
        out_specs=(
            pl.BlockSpec((4, cells, TILE, depth), lambda j: (0, 0, j, 0)),
            whole(BINS, observers),
        ),
        scratch_shapes=[
            VMEM((3, cells, width + 2 * TILE, depth), jnp.float32),
            VMEM((5, cells, TILE, depth), jnp.float32),
            VMEM((5, cells * width, depth), jnp.float32),
            VMEM((5, faces, depth), jnp.float32),
        ],
        compiler_params=pltpu.CompilerParams(**params),
    )(
        row, table,
        state, mean_flow, *received,
        z_rates, geometry,
        observer_pos, time_bin,
    )
    devices = blocks * groups
    share = observers // devices
    signal = pl.pallas_call(
        functools.partial(signal_kernel, groups, devices),
        out_shape=jax.ShapeDtypeStruct((share, BINS), jnp.float32),
        in_specs=[pl.BlockSpec(memory_space=VMEM)],
        out_specs=pl.BlockSpec(memory_space=VMEM),
        scratch_shapes=[
            VMEM((devices - 1, share, BINS), jnp.float32),
            pltpu.SemaphoreType.DMA((devices - 1,)),
            pltpu.SemaphoreType.DMA((devices - 1,)),
        ],
        compiler_params=pltpu.CompilerParams(collective_id=1, has_side_effects=True),
    )(signal.T.reshape(devices, share, BINS))
    return state_next, signal


def solution(mesh):
    in_specs = (
        P(None, "gx", "yz", None),
        P("gx", "yz", None),
        P(("gx", "yz")),
        P(None, ("gx", "yz")),
        P(None, ("gx", "yz")),
        P(),
        P(("gx", "yz"), None),
    )
    out_specs = (P(None, "gx", "yz", None), P(("gx", "yz"), None))
    sizes = (mesh.shape["gx"], mesh.shape["yz"])
    return jax.shard_map(
        functools.partial(per_device, sizes),
        mesh=mesh, in_specs=in_specs, out_specs=out_specs, check_vma=False,
    )
```
